32 devices in a mesh: dp: 8 (over y, x, core), mp: 4 (over z).
Axes of the slice: x: 2, y: 2, z: 4, core: 2. Of those that a mesh axis runs over, the one named last changes fastest.
Arguments:
- grad_parts: bfloat16 [8, 4, 1024, 4096], P('dp', None, None, 'mp'), may hold values from -4000 to 4000
- master: float32 [4, 1024, 4096], P(None, 'dp', 'mp'), may hold values from -6 to 6
- first_moment: float32 [4, 1024, 4096], P(None, 'dp', 'mp'), may hold values from -4 to 4
- second_moment: float32 [4, 1024, 4096], P(None, 'dp', 'mp'), may hold values from 0.25 to 4
- left_basis: bfloat16 [4, 1024, 4096], P(None, 'dp', 'mp'), may hold values from -1 to 1, as said below
- right_basis: bfloat16 [4, 1024, 4096], P(None, 'dp', 'mp'), may hold values from -1 to 1, as said below
Outputs:
- weights: bfloat16 [4, 1024, 4096], P(None, None, 'mp')
- new_master: float32 [4, 1024, 4096], P(None, 'dp', 'mp')
- new_first: float32 [4, 1024, 4096], P(None, 'dp', 'mp')
- new_second: float32 [4, 1024, 4096], P(None, 'dp', 'mp')
The draws below stay inside these ranges and needn't reach their ends.
Inputs may be any that keep to these rules, and one draw needn't show every extreme that they name: Each block left_basis[i, :, j * 1024 : (j + 1) * 1024] is an orthogonal 1024 x 1024 matrix up to rounding. Each block right_basis[i, :, j * 1024 : (j + 1) * 1024] is an orthogonal 1024 x 1024 matrix up to rounding.
All inputs are finite; a program needn't handle non-finite values.
Results may differ from the reference program's by a relative error of at most 0.02.
Values may be sent and summed in bfloat16 or wider, within the bound.
A program may use at most 128 MiB of HBM per device.

```python
import math
import jax
import jax.numpy as jnp
from jax import lax

D = 4096
BLK = 1024
STEP = 10
NB = 4
N_DP = 8


def orthogonal_blocks(key):
    block_count = D // BLK
    normal_part = jax.random.normal(key, (block_count, block_count, BLK, BLK), jnp.float32)
    factors = jnp.linalg.qr(normal_part)
    return factors[0].transpose(0, 2, 1, 3).reshape(block_count, BLK, D).astype(jnp.bfloat16)


def draw_left_basis(key, part):
    return orthogonal_blocks(jax.random.fold_in(key, 21))


def draw_right_basis(key, part):
    return orthogonal_blocks(jax.random.fold_in(key, 22))


def draw_grad_parts(key, part):
    subkeys = jax.random.split(jax.random.fold_in(key, 11), 5)
    places = jnp.arange(D, dtype=jnp.float32) / D
    row_scale = 10.0 ** (places + 0.3 * jax.random.uniform(subkeys[0], (D,), jnp.float32) - 0.15)
    column_scale = 10.0 ** (places + 0.3 * jax.random.uniform(subkeys[1], (D,), jnp.float32) - 0.15)
    normal_part = jax.random.normal(subkeys[4], (N_DP, D, D), jnp.float32)
    scaled = normal_part * row_scale[None, :, None] * column_scale[None, None, :]
    return scaled.reshape(N_DP, D // BLK, BLK, D).astype(jnp.bfloat16)


def level_of(stream_key, extent, cuts, least, top_value):
    factor_of = 1.0
    for position, blocks in cuts:
        steps = jax.random.uniform(jax.random.fold_in(jax.random.fold_in(stream_key, 6), position), (blocks,), jnp.float32, least / len(cuts), top_value / len(cuts))
        factor_of = factor_of * jnp.repeat(jnp.exp(steps), extent[position] // blocks).reshape((-1,) + (1,) * (len(extent) - 1 - position))
    return factor_of


def scatter_about(rng, shape, width, reach, cuts=(), held_as=jnp.bfloat16):
    entries = jax.random.normal(rng, shape, jnp.float32) * width
    if len(cuts) > 0:
        entries = level_of(rng, shape, cuts, -0.22, 0.18) * entries
    return jnp.clip(entries, min=-reach, max=reach).astype(held_as)


def setup_inputs(seed: int = 0) -> dict:
    splits = jax.random.split(jax.random.key(seed), 7)
    grad_parts = draw_grad_parts(jax.random.fold_in(splits[6], 71), 0)
    master = scatter_about(splits[1], (NB, BLK, D), 1.0, 6.0, ((1, 8), (2, 4)), jnp.float32)
    first_moment = scatter_about(splits[2], (NB, BLK, D), 0.5, 4.0, ((1, 8), (2, 4)), jnp.float32)
    second_moment = jnp.clip(jnp.exp(math.log(4.0) - 2.7725887 * jax.random.uniform(splits[3], (NB, BLK, D), jnp.float32) ** level_of(splits[3], (NB, BLK, D), ((1, 8), (2, 4)), -0.2, 0.2)), 0.25, 4.0)
    left_basis = draw_left_basis(jax.random.fold_in(splits[6], 71), 0)
    right_basis = draw_right_basis(jax.random.fold_in(splits[6], 71), 0)
    return dict(grad_parts=grad_parts, master=master, first_moment=first_moment, second_moment=second_moment, left_basis=left_basis, right_basis=right_basis)


beta_one = 0.95
beta_two = 0.95
epsilon = 1e-08
norm_epsilon = 1e-06
learning_rate = 0.3
decay_rate = 0.1

def reference(grad_parts, master, first_moment, second_moment, left_basis, right_basis):

    def add_part(running_sum, partial_value):
        return (running_sum + partial_value.astype(jnp.float32).reshape(D, D), None)
    gradient, unused_out = lax.scan(add_part, jnp.zeros((D, D), jnp.float32), grad_parts)
    squares_sum = jnp.sum(gradient * gradient)
    clip_scale = jnp.minimum(1.0, 2.0 * D / jnp.sqrt(squares_sum + norm_epsilon))
    grad_low = gradient.astype(jnp.bfloat16)
    master_flat = master.reshape(D, D)
    first_flat = first_moment.reshape(D, D)
    second_flat = second_moment.reshape(D, D)
    left_flat = left_basis.reshape(D, D)
    right_flat = right_basis.reshape(D, D)
    owner_rows = BLK // N_DP
    group_size = N_DP
    block_count = D // BLK
    bias_one = 1.0 - beta_one ** STEP
    bias_two = 1.0 - beta_two ** STEP
    master_rows, first_rows, second_rows = ([], [], [])
    for block_row in range(block_count):
        master_cols, first_cols, second_cols = ([], [], [])
        for block_column in range(block_count):
            row_span = slice(block_row * BLK, (block_row + 1) * BLK)
            column_span = slice(block_column * BLK, (block_column + 1) * BLK)
            grad_block = grad_low[row_span, column_span]
            left_block = left_flat[row_span, column_span]
            right_block = right_flat[row_span, column_span]
            turned = jnp.dot(grad_block.astype(jnp.float32), right_block.astype(jnp.float32), preferred_element_type=jnp.float32).astype(jnp.bfloat16)
            block_terms = jnp.einsum('gra,grb->gab', left_block.reshape(group_size, owner_rows, BLK).astype(jnp.float32), turned.reshape(group_size, owner_rows, BLK).astype(jnp.float32))
            rounded_terms = lax.optimization_barrier(block_terms.astype(jnp.bfloat16))
            rotated = lax.optimization_barrier(jnp.sum(rounded_terms.astype(jnp.float32), axis=0))
            clipped = clip_scale * rotated
            first_new = beta_one * first_flat[row_span, column_span] + (1.0 - beta_one) * clipped
            second_new = beta_two * second_flat[row_span, column_span] + (1.0 - beta_two) * clipped * clipped
            direction = (first_new / bias_one / (jnp.sqrt(second_new / bias_two) + epsilon)).astype(jnp.bfloat16)
            back_rows = jnp.dot(direction.astype(jnp.float32), right_block.T.astype(jnp.float32), preferred_element_type=jnp.float32).astype(jnp.bfloat16)
            update = jnp.dot(left_block.astype(jnp.float32), back_rows.astype(jnp.float32), preferred_element_type=jnp.float32)
            master_new = master_flat[row_span, column_span] * (1.0 - learning_rate * decay_rate) - learning_rate * update
            master_cols.append(master_new)
            first_cols.append(first_new)
            second_cols.append(second_new)
        master_rows.append(jnp.concatenate(master_cols, axis=1))
        first_rows.append(jnp.concatenate(first_cols, axis=1))
        second_rows.append(jnp.concatenate(second_cols, axis=1))
    new_master = jnp.concatenate(master_rows, axis=0).reshape(D // BLK, BLK, D)
    new_first = jnp.concatenate(first_rows, axis=0).reshape(D // BLK, BLK, D)
    new_second = jnp.concatenate(second_rows, axis=0).reshape(D // BLK, BLK, D)
    return (new_master.astype(jnp.bfloat16), new_master, new_first, new_second)
```

```python
import functools

import jax
import jax.numpy as jnp
from jax import lax
from jax.experimental import pallas as pl
from jax.experimental.pallas import tpu as pltpu
from jax.sharding import PartitionSpec as P

D = 4096
STEP = 10


beta_one = 0.95
beta_two = 0.95
epsilon = 1e-08
norm_epsilon = 1e-06
learning_rate = 0.3
decay_rate = 0.1

VMEM = pl.BlockSpec(memory_space=pltpu.VMEM)
MESH = pl.DeviceIdType.MESH


def remote(src, dst, send, recv, axis, index):
    return pltpu.make_async_remote_copy(
        src_ref=src,
        dst_ref=dst,
        send_sem=send,
        recv_sem=recv,
        device_id={axis: index},
        device_id_type=MESH,
    )


def enter(axes):
    barrier = pltpu.get_barrier_semaphore()
    total = 0
    for axis, size in axes:
        me = lax.axis_index(axis)
        for step in range(1, size):
            pl.semaphore_signal(
                barrier,
                inc=1,
                device_id={axis: lax.rem(me + step, size)},
                device_id_type=MESH,
            )
        total += size - 1
    pl.semaphore_wait(barrier, total)


class Gather:
    def __init__(self, n, nb, x, y, local, first, recv, second):
        self.n, self.nb, self.q = n, nb, n // nb
        self.x, self.y = x, y
        self.local, self.first, self.recv, self.second = local, first, recv, second
        self.me = lax.axis_index("dp")
        self.g, self.r = self.me // self.q, lax.rem(self.me, self.q)
        self.sent = []

    def go(self, src, slot, send, target):
        copy = remote(src, self.y.at[slot], send, self.recv.at[slot], "dp", target)
        copy.start()
        self.sent.append(copy)

    def arrived(self, slot):
        remote(
            self.y.at[slot], self.y.at[slot], self.first.at[0], self.recv.at[slot], "dp", self.me
        ).wait_recv()

    def start(self):
        nb, q, me, g, r = self.nb, self.q, self.me, self.g, self.r
        for j in range(1, nb):
            other = lax.rem(g + j, nb)
            self.go(self.x.at[other], me, self.first.at[j], other * q + r)
        for p in range(1, q):
            self.go(self.x.at[g], me, self.second.at[p], g * q + lax.rem(r + p, q))
        self.own = pltpu.make_async_copy(self.x.at[g], self.y.at[me], self.local.at[0])
        self.own.start()

    def forward(self):
        nb, q, g, r = self.nb, self.q, self.g, self.r
        for j in range(1, nb):
            slot = lax.rem(g + nb - j, nb) * q + r
            self.arrived(slot)
            for p in range(1, q):
                self.go(
                    self.y.at[slot], slot, self.second.at[j * q + p], g * q + lax.rem(r + p, q)
                )

    def finish(self):
        nb, q, r = self.nb, self.q, self.r
        self.own.wait()
        for p in range(1, q):
            for j in range(nb):
                self.arrived(j * q + lax.rem(r + p, q))
        for copy in self.sent:
            copy.wait_send()

    @staticmethod
    def scratch(n, nb):
        return [
            pltpu.SemaphoreType.DMA((1,)),
            pltpu.SemaphoreType.DMA((nb,)),
            pltpu.SemaphoreType.DMA((n,)),
            pltpu.SemaphoreType.DMA((n,)),
        ]


class Exchange:
    def __init__(self, n, nb, to_rows, x, y, local, send, recv):
        q = n // nb
        me = lax.axis_index("dp")
        self.nb, self.x, self.y = nb, x, y
        self.local, self.send, self.recv, self.me = local, send, recv, me
        owner = lax.rem(me, q) * nb
        first = me // nb
        if to_rows:
            self.targets = [owner + k for k in range(nb)]
            self.slot = me // q
            self.sources = [k * q + first for k in range(nb)]
        else:
            self.targets = [k * q + first for k in range(nb)]
            self.slot = lax.rem(me, nb)
            self.sources = [owner + k for k in range(nb)]

    def copy(self, k):
        return remote(
            self.x.at[k],
            self.y.at[self.slot],
            self.send.at[k],
            self.recv.at[self.slot],
            "dp",
            self.targets[k],
        )

    def mine(self, k):
        return pltpu.make_async_copy(self.x.at[k], self.y.at[self.slot], self.local.at[0])

    def start(self):
        for k in range(self.nb):

            @pl.when(self.targets[k] != self.me)
            def _():
                self.copy(k).start()

            @pl.when(self.targets[k] == self.me)
            def _():
                self.mine(k).start()

    def finish(self):
        for k in range(self.nb):

            @pl.when(self.sources[k] != self.me)
            def _():
                remote(
                    self.y.at[k], self.y.at[k], self.send.at[k], self.recv.at[k], "dp", self.me
                ).wait_recv()

            @pl.when(self.targets[k] != self.me)
            def _():
                self.copy(k).wait_send()

            @pl.when(self.targets[k] == self.me)
            def _():
                self.mine(k).wait()

    @staticmethod
    def scratch(nb):
        return [
            pltpu.SemaphoreType.DMA((1,)),
            pltpu.SemaphoreType.DMA((nb,)),
            pltpu.SemaphoreType.DMA((nb,)),
        ]


class Share:
    def __init__(self, axis, size, x, y, local, send, recv):
        self.axis, self.size, self.x, self.y = axis, size, x, y
        self.local, self.send, self.recv = local, send, recv
        self.me = lax.axis_index(axis)

    def copy(self, j):
        return remote(
            self.x,
            self.y.at[self.me],
            self.send.at[j],
            self.recv.at[self.me],
            self.axis,
            lax.rem(self.me + j, self.size),
        )

    def start(self):
        for j in range(1, self.size):
            self.copy(j).start()
        self.own = pltpu.make_async_copy(self.x, self.y.at[self.me], self.local.at[0])
        self.own.start()

    def finish(self):
        self.own.wait()
        for j in range(1, self.size):
            slot = lax.rem(self.me + j, self.size)
            remote(
                self.y.at[slot], self.y.at[slot], self.send.at[j], self.recv.at[slot], self.axis, slot
            ).wait_recv()
        for j in range(1, self.size):
            self.copy(j).wait_send()

    @staticmethod
    def scratch(size):
        return [
            pltpu.SemaphoreType.DMA((1,)),
            pltpu.SemaphoreType.DMA((size,)),
            pltpu.SemaphoreType.DMA((size,)),
        ]


def bases_kernel(n, nb, left, right, master, left_out, right_out, master_out, *sems):
    enter([("dp", n)])
    one = Gather(n, nb, right, right_out, *sems[0:4])
    two = Gather(n, nb, left, left_out, *sems[4:8])
    three = Exchange(n, nb, False, master, master_out, *sems[8:11])
    one.start()
    two.start()
    three.start()
    one.forward()
    two.forward()
    one.finish()
    two.finish()
    three.finish()


def gather_kernel(n, nb, x, y, *sems):
    enter([("dp", n)])
    one = Gather(n, nb, x, y, *sems)
    one.start()
    one.forward()
    one.finish()


def scatter_kernel(n, nb, x, y, *sems):
    enter([("dp", n)])
    one = Exchange(n, nb, True, x, y, *sems)
    one.start()
    one.finish()


def scatter_sum_kernel(n, m, nb, x, part, y, parts, *sems):
    enter([("dp", n), ("mp", m)])
    two = Share("mp", m, part, parts, *sems[3:6])
    two.start()
    one = Exchange(n, nb, True, x, y, *sems[0:3])
    one.start()
    two.finish()
    one.finish()


def group_kernel(n, nb, x, part, y, parts, *sems):
    enter([("dp", n)])
    q = n // nb
    me = lax.axis_index("dp")
    g, r = me // q, lax.rem(me, q)
    local, send, recv = sems[0:3]
    copies = []
    for p in range(1, q):
        copy = remote(
            x, y.at[r], send.at[p], recv.at[r], "dp", g * q + lax.rem(r + p, q)
        )
        copy.start()
        copies.append(copy)
    two = Share("dp", n, part, parts, *sems[3:6])
    two.start()
    own = pltpu.make_async_copy(x, y.at[r], local.at[0])
    own.start()
    own.wait()
    for p in range(1, q):
        slot = lax.rem(r + p, q)
        remote(y.at[slot], y.at[slot], send.at[p], recv.at[slot], "dp", me).wait_recv()
    two.finish()
    for copy in copies:
        copy.wait_send()


def call(kernel, shapes, scratch, collective_id, *args):
    moved = sum(s.size * s.dtype.itemsize for s in shapes)
    return pl.pallas_call(
        kernel,
        out_shape=shapes,
        in_specs=[VMEM] * len(args),
        out_specs=[VMEM] * len(shapes),
        scratch_shapes=scratch,
        compiler_params=pltpu.CompilerParams(
            collective_id=collective_id, has_side_effects=True, vmem_limit_bytes=32 * 1024 * 1024
        ),
        cost_estimate=pl.CostEstimate(flops=0, bytes_accessed=16 * moved, transcendentals=0),
    )(*args)


def per_device(n, m, grad_parts, master, first_moment, second_moment, left_basis, right_basis):
    bf16, f32 = jnp.bfloat16, jnp.float32
    nb, rb, cols = master.shape
    blk = rb * n
    q = n // nb
    hb = blk // q
    r = lax.rem(lax.axis_index("dp"), q)
    pieces = jax.ShapeDtypeStruct((nb, rb, cols), bf16)
    block = jax.ShapeDtypeStruct((n, rb, cols), bf16)
    low_sum = lax.psum_scatter(
        grad_parts.reshape(nb * blk, cols), "dp", scatter_dimension=0, tiled=True
    )
    left, right, master_low = call(
        functools.partial(bases_kernel, n, nb),
        [block, block, pieces],
        Gather.scratch(n, nb) * 2 + Exchange.scratch(nb),
        0,
        left_basis,
        right_basis,
        master.astype(bf16),
    )
    left, right = left.reshape(blk, cols), right.reshape(blk, cols)
    left_cols = lax.dynamic_slice_in_dim(left, r * hb, hb, axis=1)
    left_rows = lax.dynamic_slice_in_dim(left, r * hb, hb, axis=0)
    gradient = low_sum.astype(f32)
    part = jnp.full((8, 128), jnp.sum(gradient * gradient), f32)
    grad_block, parts = call(
        functools.partial(group_kernel, n, nb),
        [
            jax.ShapeDtypeStruct((q, hb, cols), bf16),
            jax.ShapeDtypeStruct((n, 8, 128), f32),
        ],
        Share.scratch(q) + Share.scratch(n),
        1,
        low_sum,
        part,
    )
    part = jnp.sum(parts, axis=0)
    turned = jnp.dot(
        grad_block.reshape(blk, cols), right, preferred_element_type=f32
    ).astype(bf16)
    rotated_rows = lax.dot_general(
        left_cols, turned, (((0,), (0,)), ((), ())), preferred_element_type=f32
    ).astype(bf16)
    rotated, parts = call(
        functools.partial(scatter_sum_kernel, n, m, nb),
        [pieces, jax.ShapeDtypeStruct((m, 8, 128), f32)],
        Exchange.scratch(nb) + Share.scratch(m),
        2,
        rotated_rows.reshape(nb, rb, cols),
        part,
    )
    squares_sum = jnp.sum(parts[:, 0, 0])
    clip_scale = jnp.minimum(1.0, 2.0 * D / jnp.sqrt(squares_sum + norm_epsilon))
    clipped = clip_scale * rotated.astype(f32)
    new_first = beta_one * first_moment + (1.0 - beta_one) * clipped
    new_second = beta_two * second_moment + (1.0 - beta_two) * clipped * clipped
    bias_one = 1.0 - beta_one**STEP
    bias_two = 1.0 - beta_two**STEP
    direction = (new_first / bias_one / (jnp.sqrt(new_second / bias_two) + epsilon)).astype(bf16)
    (direction_block,) = call(
        functools.partial(gather_kernel, n, nb), [block], Gather.scratch(n, nb), 3, direction
    )
    back = lax.dot_general(
        direction_block.reshape(blk, cols),
        right,
        (((1,), (1,)), ((), ())),
        preferred_element_type=f32,
    ).astype(bf16)
    update = jnp.dot(left_rows, back, preferred_element_type=f32)
    keep = 1.0 - learning_rate * decay_rate
    weight_rows = (
        master_low.reshape(hb, cols).astype(f32) * keep - learning_rate * update
    ).astype(bf16)
    weights = lax.all_gather(weight_rows, "dp", axis=0, tiled=True).reshape(nb, blk, cols)
    (update_rows,) = call(
        functools.partial(scatter_kernel, n, nb),
        [pieces],
        Exchange.scratch(nb),
        4,
        update.astype(bf16).reshape(nb, rb, cols),
    )
    new_master = master * keep - learning_rate * update_rows.astype(f32)
    return (weights, new_master, new_first, new_second)


def solution(mesh):
    n, m = mesh.shape["dp"], mesh.shape["mp"]
    return jax.shard_map(
        functools.partial(per_device, n, m),
        mesh=mesh,
        in_specs=(
            P("dp", None, None, "mp"),
            P(None, "dp", "mp"),
            P(None, "dp", "mp"),
            P(None, "dp", "mp"),
            P(None, "dp", "mp"),
            P(None, "dp", "mp"),
        ),
        out_specs=(
            P(None, None, "mp"),
            P(None, "dp", "mp"),
            P(None, "dp", "mp"),
            P(None, "dp", "mp"),
        ),
        check_vma=False,
    )
```
